32 devices in a mesh: groups: 2 (over x), lat: 16 (over z, y, core).
Axes of the slice: x: 2, y: 2, z: 4, core: 2. Of those that a mesh axis runs over, the one named last changes fastest.
Arguments:
- inputs: bfloat16 [1024, 4608], P('groups', 'lat'), parts along dimension 0, may hold values from -6 to 6
- w_enc: bfloat16 [9216, 8192], P('groups', 'lat'), parts along dimension 0, may hold values from -0.09375 to 0.09375
- b_enc: float32 [16384], P(('groups', 'lat')), parts along dimension 0, may hold values from -3 to 3
- thresholds: float32 [16384], P(('groups', 'lat')), parts along dimension 0, may hold values from 0.1 to 4
- w_dec: bfloat16 [16384, 4608], P(('groups', 'lat')), parts along dimension 0, may hold values from -0.1875 to 0.1875
- b_dec: bfloat16 [9216], P(('groups', 'lat')), parts along dimension 0, may hold values from -5 to 5
- sparsity: float32 [2], P('groups'), parts along dimension 0, may hold values from 1 to 4
Outputs:
- grad_enc: bfloat16 [9216, 8192], P('groups', 'lat'), parts along dimension 0
- grad_b_enc: float32 [16384], P(('groups', 'lat')), parts along dimension 0
- grad_dec: bfloat16 [16384, 4608], P(('groups', 'lat')), parts along dimension 0
- grad_b_dec: float32 [9216], P(('groups', 'lat')), parts along dimension 0
- loss_terms: float32 [4], P('groups'), parts along dimension 0
The draws below stay inside these ranges and needn't reach their ends.
There are 2 independent parts, one for each index of `groups`. The reference program is written for one: setup_inputs(seed, part) draws one part's arguments, and reference() takes and returns one part's arrays. A program takes and returns all parts, laid end to end along the dimension named above; each array names one. Nothing has to cross between parts.
All inputs are finite; a program needn't handle non-finite values.
Results may differ from the reference program's by a relative error of at most 0.006.
Values may be sent and summed in bfloat16 or wider, within the bound.
A program may use at most 128 MiB of HBM per device.

```python
import math
import jax
import jax.numpy as jnp
from jax import lax

D = 4608
LAT_DEV = 512
ROWS = 512
LATENTS = 8192


def draw_thresholds(key, part):
    blocks = LATENTS // LAT_DEV
    key_level = jax.random.fold_in(key, 11)
    key_inner = jax.random.fold_in(key, 23)
    key_pick = jax.random.fold_in(key, 37)
    levels = jnp.exp(jax.random.uniform(key_level, (blocks, 1), jnp.float32, math.log(0.25), math.log(2.5)))
    chosen = jax.random.randint(key_pick, (), 0, blocks)
    levels = jnp.where(jnp.arange(blocks).reshape(blocks, 1) == chosen, jnp.float32(0.25), levels)
    inner = jnp.exp(jax.random.uniform(key_inner, (blocks, LAT_DEV), jnp.float32, math.log(0.4), math.log(1.6)))
    return (levels * inner).reshape(LATENTS).astype(jnp.float32)


def with_spikes(values, own_key, source, target, shards_of, factor):
    owner, partner = [(jnp.arange(values.shape[dim]) // (values.shape[dim] // shards_of)).reshape([-1 if axis == dim else 1 for axis in range(values.ndim)]) for dim in (source, target)]
    chosen = jax.random.permutation(own_key, shards_of)[partner]
    strong = (owner == chosen) | (owner == (partner + shards_of // 2) % shards_of)
    return jnp.where(strong, factor * values, values)


def level_of(stream_key, shape, shards, least, high):
    level = 1.0
    for position, shards_of in shards:
        draws = jax.random.uniform(jax.random.fold_in(jax.random.fold_in(stream_key, 6), position), (shards_of,), jnp.float32, least / len(shards), high / len(shards))
        level = level * jnp.repeat(jnp.exp(draws), shape[position] // shards_of).reshape((-1,) + (1,) * (len(shape) - 1 - position))
    return level


def normal_values(stream_key, extent, deviation, bound, shards=(), held_as=jnp.bfloat16):
    array = deviation * jax.random.normal(stream_key, extent, jnp.float32)
    if shards:
        array = array * level_of(stream_key, extent, shards, -0.22, 0.18)
    return jnp.clip(array, -bound, bound).astype(held_as)


def gaussian_with(rng, shape, deviation, reach, cuts, heavy, kind=jnp.bfloat16):
    entries = deviation * jax.random.normal(rng, shape, jnp.float32)
    if cuts:
        entries = entries * level_of(rng, shape, cuts, -0.22, 0.18)
    return jnp.clip(with_spikes(entries, jax.random.fold_in(rng, 3), *heavy), -reach, reach).astype(kind)


def setup_inputs(seed: int = 0, part: int = 0) -> dict:
    splits = jax.random.split(jax.random.key(seed), 8)
    own_keys = jax.random.split(jax.random.fold_in(splits[7], part), 8)
    return {
        "inputs": normal_values(own_keys[0], (ROWS, D), 1.0, 6.0, ((1, 16),)),
        "w_enc": normal_values(own_keys[1], (D, LATENTS), D ** -0.5, 0.09375, ((1, 16),)),
        "b_enc": normal_values(own_keys[2], (LATENTS,), 0.5, 3.0, ((0, 16),), jnp.float32),
        "thresholds": draw_thresholds(jax.random.fold_in(jax.random.fold_in(splits[7], part), 71), part),
        "w_dec": gaussian_with(own_keys[4], (LATENTS, D), (LATENTS // 4) ** -0.5, 0.1875, ((0, 16),), (0, 1, 16, 2.0)),
        "b_dec": normal_values(own_keys[5], (D,), 1.0, 5.0, ((0, 16),)),
        "sparsity": jnp.clip(jax.random.uniform(own_keys[6], (1,), jnp.float32, 1.0, 4.0), 1.0, 4.0),
    }


def reference(inputs, w_enc, b_enc, thresholds, w_dec, b_dec, sparsity):
    rows = inputs.shape[0]
    pre = jnp.dot(inputs, w_enc, preferred_element_type=jnp.float32) + b_enc
    gate = jax.nn.sigmoid((pre - thresholds) / 0.05)
    feats = (pre * gate).astype(jnp.bfloat16)
    recon = jnp.dot(feats, w_dec, preferred_element_type=jnp.float32) + b_dec.astype(jnp.float32)
    err = recon - inputs.astype(jnp.float32)
    scaled = (2.0 / rows) * err
    error_bf = scaled.astype(jnp.bfloat16)
    grad_b_dec = jnp.sum(scaled, axis=0)
    grad_dec = lax.dot_general(feats, error_bf, (((0,), (0,)), ((), ())), preferred_element_type=jnp.float32).astype(jnp.bfloat16)
    g_feats = lax.dot_general(error_bf, w_dec, (((1,), (1,)), ((), ())), preferred_element_type=jnp.float32)
    g_pre = g_feats * (gate + pre * gate * (1.0 - gate) / 0.05)
    g_pre_bf = g_pre.astype(jnp.bfloat16)
    grad_b_enc = jnp.sum(g_pre, axis=0)
    grad_enc = lax.dot_general(inputs, g_pre_bf, (((0,), (0,)), ((), ())), preferred_element_type=jnp.float32).astype(jnp.bfloat16)
    loss_terms = jnp.stack([jnp.sum(err * err) / (rows * D), sparsity[0] * jnp.sum(gate) / (rows * LATENTS)])
    return grad_enc, grad_b_enc, grad_dec, grad_b_dec, loss_terms
```

```python
import functools

import jax
import jax.numpy as jnp
from jax import lax
from jax.experimental import pallas as pl
from jax.experimental.pallas import tpu as pltpu
from jax.sharding import PartitionSpec as P

MESH = pl.DeviceIdType.MESH
F32 = jnp.float32
BF16 = jnp.bfloat16


def dot(a, b, ca, cb):
    return lax.dot_general(a, b, (((ca,), (cb,)), ((), ())), preferred_element_type=F32)


def step_kernel(
    n, inner, rows_total,
    x_ref, wenc_hbm, wdec_hbm, benc_ref, thr_ref, bdec_ref,
    xt_hbm, et_hbm, ft_ref, gp_ref, gbenc_ref, gbdec_ref, stats_ref,
    xt, et, wenc, wdec, wdt, pre, dg, theirs, given, mine, sbuf, rbuf, st,
    load_sem, out_sem,
    a_ss, a_rs, a_ds, a_dr, r_ss, r_rs, r_ds, r_dr, e_ss, e_rs, e_ds, e_dr,
):
    blk, half = x_ref.shape[1], x_ref.shape[2]
    depth, lat = wenc.shape
    subs = 2 if blk % 32 == 0 else 1
    sub_rows = blk // subs
    me = lax.axis_index("lat")
    core = lax.rem(me, 2)
    chip = me // 2
    m = n // 2

    if inner == 2:
        y0 = lax.rem(chip, 2)
        z0 = chip // 2
        pos = z0 + y0 * (2 * m - 1 - 2 * z0)
    else:
        pos = chip

    def chip_at(p):
        p = lax.rem(p + 2 * n, n)
        if inner == 2:
            y = p // m
            z = p + y * (2 * m - 1 - 2 * p)
            return 2 * z + y
        return p

    nxt = 2 * chip_at(pos + 1) + core
    prv = 2 * chip_at(pos - 1) + core
    mate = me + 1 - 2 * core

    barrier = pltpu.get_barrier_semaphore()
    for peer in (nxt, prv, mate):
        pl.semaphore_signal(barrier, inc=1, device_id={"lat": peer}, device_id_type=MESH)

    own_rows = pl.ds(pl.multiple_of(me * blk, 16), blk)
    load_enc = pltpu.make_async_copy(wenc_hbm, wenc, load_sem.at[0])
    load_dec = pltpu.make_async_copy(wdec_hbm, wdec, load_sem.at[1])
    load_x = pltpu.make_async_copy(x_ref, xt.at[:, own_rows], load_sem.at[2])
    load_x.start()
    load_enc.start()
    load_dec.start()
    load_x.wait()
    pl.semaphore_wait(barrier, 3)

    def remote(src, dst, ss, rs, peer):
        return pltpu.make_async_remote_copy(
            src_ref=src, dst_ref=dst, send_sem=ss, recv_sem=rs,
            device_id={"lat": peer}, device_id_type=MESH,
        )

    def make_gather(buf, with_stats, ss, rs, ds, dr):
        flows = [(h, u) for h in range(2) for u in range(subs)]
        if with_stats:
            flows.append((0, -1))

        def piece(f, dev):
            h, u = flows[f]
            if u < 0:
                return st.at[dev]
            return buf.at[h, pl.ds(pl.multiple_of(dev * blk + u * sub_rows, 16), sub_rows)]

        def dev_at(f, s, c):
            sign = 1 if flows[f][0] == 0 else -1
            return 2 * chip_at(pos - sign * s) + c

        def ring(f, s):
            r = piece(f, dev_at(f, s, core))
            return remote(r, r, ss.at[f, s], rs.at[f, s], nxt if flows[f][0] == 0 else prv)

        def ring_in(f, s):
            r = piece(f, dev_at(f, s + 1, core))
            return remote(r, r, ss.at[f, s], rs.at[f, s], nxt if flows[f][0] == 0 else prv)

        def d2d(f, s):
            r = piece(f, dev_at(f, s, core))
            return remote(r, r, ds.at[f, s], dr.at[f, s], mate)

        def d2d_in(f, s):
            r = piece(f, dev_at(f, s, 1 - core))
            return remote(r, r, ds.at[f, s], dr.at[f, s], mate)

        count = range(len(flows))

        def run(first, compute):
            for f in count:
                ring(f, 0).start()
            for f in count:
                d2d(f, 0).start()
            first()

            def arrive(s):
                for f in count:
                    d2d_in(f, s).wait_recv()

            @pl.loop(1, n - 1)
            def _(s):
                for f in count:
                    ring_in(f, s - 1).wait_recv()
                    ring(f, s).start()
                    d2d(f, s).start()
                arrive(s - 1)
                compute(s - 1)

            for f in count:
                ring_in(f, n - 2).wait_recv()
                d2d(f, n - 1).start()
            arrive(n - 2)
            compute(n - 2)
            arrive(n - 1)
            compute(n - 1)

            @pl.loop(0, n - 1)
            def _(s):
                for f in count:
                    ring(f, s).wait_send()

            @pl.loop(0, n)
            def _(s):
                for f in count:
                    d2d(f, s).wait_send()

        return run

    def first():
        pre[...] = jnp.zeros_like(pre)
        load_dec.wait()

        @pl.loop(0, depth // 128)
        def _(i):
            c = pl.ds(pl.multiple_of(i * 128, 128), 128)
            wdt[c, :] = wdec[:, c].T

        load_enc.wait()

    def encode(s):
        for h in range(2):
            q = chip_at(pos - s if h == 0 else pos + s)
            r = pl.ds(pl.multiple_of(q * 2 * blk, 16), 2 * blk)
            pre[h] += dot(wenc[r, :], xt[h, r, :], 0, 0)

    make_gather(xt, False, a_ss, a_rs, a_ds, a_dr)(first, encode)
    out_x = pltpu.make_async_copy(xt, xt_hbm, out_sem.at[0])
    out_x.start()

    total = jnp.zeros((1, half), F32)
    for h in range(2):
        p = pre[h] + benc_ref[...]
        gate = jax.nn.sigmoid((p - thr_ref[...]) / 0.05)
        ft_ref[h] = (p * gate).astype(BF16)
        dg[h] = gate + p * gate * (1.0 - gate) / 0.05
        total = total + jnp.sum(gate, axis=0, keepdims=True)

    def block_at(h, t):
        return chip_at(pos - 1 - t if h == 0 else pos + 1 + t)

    def swap(h, t):
        return remote(theirs.at[h, t], given.at[h, t], r_ds.at[h, t], r_dr.at[h, t], mate)

    def partial(t):
        for h in range(2):
            q = block_at(h, t)
            other = pl.ds(pl.multiple_of((2 * q + 1 - core) * blk, 16), blk)
            theirs[h, t] = dot(wdt[other, :], ft_ref[h], 1, 0).astype(BF16)
            swap(h, t).start()
        for h in range(2):
            q = block_at(h, t)
            same = pl.ds(pl.multiple_of((2 * q + core) * blk, 16), blk)
            mine[h, t] = dot(wdt[same, :], ft_ref[h], 1, 0)

    def pass_on(h, u, s):
        r = pl.ds(u * sub_rows, sub_rows)
        f = h * subs + u
        return remote(
            sbuf.at[h, s, r], rbuf.at[h, s, r], r_ss.at[f, s], r_rs.at[f, s], nxt if h == 0 else prv
        )

    def hop(s, has_input):
        for h in range(2):
            swap(h, s).wait_recv()
        for u in range(subs):
            for h in range(2):
                r = pl.ds(u * sub_rows, sub_rows)
                v = mine[h, s, r, :] + given[h, s, r, :].astype(F32)
                if has_input:
                    pass_on(h, u, s - 1).wait_recv()
                    v = v + rbuf[h, s - 1, r, :].astype(F32)
                sbuf[h, s, r, :] = v.astype(BF16)
                pass_on(h, u, s).start()

    partial(0)
    partial(1)
    hop(0, False)
    partial(2)

    @pl.loop(1, n - 2)
    def _(s):
        hop(s, True)
        partial(s + 2)

    hop(n - 2, True)
    sq = jnp.zeros((1, half), F32)
    gb = jnp.zeros((blk, 1), F32)
    for h in range(2):
        swap(h, n - 1).wait_recv()
        for u in range(subs):
            pass_on(h, u, n - 2).wait_recv()
        recon = mine[h, n - 1] + given[h, n - 1].astype(F32) + rbuf[h, n - 2].astype(F32) + bdec_ref[...]
        err = recon - x_ref[h].astype(F32)
        scaled = (2.0 / rows_total) * err
        et[h, own_rows, :] = scaled.astype(BF16)
        sq = sq + jnp.sum(err * err, axis=0, keepdims=True)
        gb = gb + jnp.sum(scaled, axis=1, keepdims=True)
    gbdec_ref[...] = gb
    lane = lax.broadcasted_iota(jnp.int32, (8, 128), 0)
    st[me] = jnp.where(lane == 0, jnp.sum(sq), jnp.sum(total))

    def nothing(*_):
        pass

    make_gather(et, True, e_ss, e_rs, e_ds, e_dr)(nothing, nothing)
    out_e = pltpu.make_async_copy(et, et_hbm, out_sem.at[1])
    out_e.start()

    @pl.loop(0, n - 1)
    def _(s):
        for h in range(2):
            for u in range(subs):
                pass_on(h, u, s).wait_send()

    @pl.loop(0, n)
    def _(s):
        for h in range(2):
            swap(h, s).wait_send()

    chunk = next(c for c in range(1152, 0, -128) if depth % c == 0)
    gsum = jnp.zeros((lat, 1), F32)
    for h in range(2):
        pre[h] = jnp.zeros_like(pre[h])

        @pl.loop(0, depth // chunk)
        def _(i):
            c = pl.ds(pl.multiple_of(i * chunk, 128), chunk)
            pre[h] += dot(wdec[:, c], et[h, c, :], 1, 0)

        g = pre[h] * dg[h]
        gp_ref[h] = g.astype(BF16)
        gsum = gsum + jnp.sum(g, axis=1, keepdims=True)
    gbenc_ref[...] = gsum
    stats_ref[...] = jnp.sum(st[...], axis=0)
    out_x.wait()
    out_e.wait()


def grads_kernel(xt_ref, et_ref, ft_ref, gp_ref, genc_ref, gdec_ref):
    genc_ref[...] = (dot(xt_ref[0], gp_ref[0], 1, 1) + dot(xt_ref[1], gp_ref[1], 1, 1)).astype(BF16)
    gdec_ref[...] = (dot(ft_ref[0], et_ref[0], 1, 1) + dot(ft_ref[1], et_ref[1], 1, 1)).astype(BF16)


def on_device(inner, inputs, w_enc, b_enc, thresholds, w_dec, b_dec, sparsity):
    rows, blk = inputs.shape
    parts = lax.axis_size("lat")
    n = parts // 2
    depth, lat = w_enc.shape
    half = rows // 2
    subs = 2 if blk % 32 == 0 else 1
    nf = 2 * subs
    x_blocks = jnp.transpose(inputs.reshape(2, half, blk), (0, 2, 1))
    vmem = pl.BlockSpec(memory_space=pltpu.VMEM)
    hbm = pl.BlockSpec(memory_space=pl.ANY)
    dma = pltpu.SemaphoreType.DMA
    xt, et, ft, gp, gbenc, gbdec, stats = pl.pallas_call(
        functools.partial(step_kernel, n, inner, rows),
        out_shape=(
            jax.ShapeDtypeStruct((2, depth, half), BF16),
            jax.ShapeDtypeStruct((2, depth, half), BF16),
            jax.ShapeDtypeStruct((2, lat, half), BF16),
            jax.ShapeDtypeStruct((2, lat, half), BF16),
            jax.ShapeDtypeStruct((lat, 1), F32),
            jax.ShapeDtypeStruct((blk, 1), F32),
            jax.ShapeDtypeStruct((8, 128), F32),
        ),
        in_specs=[vmem, hbm, hbm, vmem, vmem, vmem],
        out_specs=(hbm, hbm, vmem, vmem, vmem, vmem, vmem),
        scratch_shapes=[
            pltpu.VMEM((2, depth, half), BF16),
            pltpu.VMEM((2, depth, half), BF16),
            pltpu.VMEM((depth, lat), BF16),
            pltpu.VMEM((lat, depth), BF16),
            pltpu.VMEM((depth, lat), BF16),
            pltpu.VMEM((2, lat, half), F32),
            pltpu.VMEM((2, lat, half), F32),
            pltpu.VMEM((2, n, blk, half), BF16),
            pltpu.VMEM((2, n, blk, half), BF16),
            pltpu.VMEM((2, n, blk, half), F32),
            pltpu.VMEM((2, n - 1, blk, half), BF16),
            pltpu.VMEM((2, n - 1, blk, half), BF16),
            pltpu.VMEM((parts, 8, 128), F32),
            dma((3,)),
            dma((2,)),
            dma((nf, n - 1)), dma((nf, n - 1)), dma((nf, n)), dma((nf, n)),
            dma((nf, n - 1)), dma((nf, n - 1)), dma((2, n)), dma((2, n)),
            dma((nf + 1, n - 1)), dma((nf + 1, n - 1)), dma((nf + 1, n)), dma((nf + 1, n)),
        ],
        compiler_params=pltpu.CompilerParams(
            collective_id=0, has_side_effects=True, vmem_limit_bytes=63 * 1024 * 1024
        ),
        name="sae_step",
    )(
        x_blocks, w_enc, w_dec, b_enc.reshape(lat, 1), thresholds.reshape(lat, 1),
        b_dec.astype(F32).reshape(blk, 1),
    )
    tile = 512 if depth % 512 == 0 else 128
    grad_enc, grad_dec = pl.pallas_call(
        grads_kernel,
        grid=(depth // tile,),
        out_shape=(
            jax.ShapeDtypeStruct((depth, lat), BF16),
            jax.ShapeDtypeStruct((lat, depth), BF16),
        ),
        in_specs=[
            pl.BlockSpec((2, tile, half), lambda i: (0, i, 0)),
            pl.BlockSpec((2, tile, half), lambda i: (0, i, 0)),
            pl.BlockSpec((2, lat, half), lambda i: (0, 0, 0)),
            pl.BlockSpec((2, lat, half), lambda i: (0, 0, 0)),
        ],
        out_specs=(
            pl.BlockSpec((tile, lat), lambda i: (i, 0)),
            pl.BlockSpec((lat, tile), lambda i: (0, i)),
        ),
        name="sae_grads",
    )(xt, et, ft, gp)
    loss_terms = jnp.stack(
        [
            stats[0, 0] / (rows * depth),
            sparsity[0] * stats[1, 0] / (rows * lat * parts),
        ]
    )
    return grad_enc, gbenc.reshape(lat), grad_dec, gbdec.reshape(blk), loss_terms


def chips_inner(mesh):
    try:
        where = [tuple(d.coords) for d in mesh.devices.reshape(-1, mesh.shape["lat"])[0][::2]]
    except AttributeError:
        return 1
    if len(where) < 4 or len(where) % 2:
        return 1
    moved = [sum(a != b for a, b in zip(where[0], w)) for w in (where[1], where[2], where[3])]
    return 2 if moved == [1, 1, 2] else 1


def solution(mesh):
    return jax.shard_map(
        functools.partial(on_device, chips_inner(mesh)),
        mesh=mesh,
        in_specs=(
            P("groups", "lat"),
            P("groups", "lat"),
            P(("groups", "lat")),
            P(("groups", "lat")),
            P(("groups", "lat"), None),
            P(("groups", "lat")),
            P("groups"),
        ),
        out_specs=(
            P("groups", "lat"),
            P(("groups", "lat")),
            P(("groups", "lat"), None),
            P(("groups", "lat")),
            P("groups"),
        ),
        check_vma=False,
    )
```

```python
import functools

import jax
import jax.numpy as jnp
from jax import lax
from jax.experimental import pallas as pl
from jax.experimental.pallas import tpu as pltpu
from jax.sharding import PartitionSpec as P

MESH = pl.DeviceIdType.MESH
F32 = jnp.float32
BF16 = jnp.bfloat16


def dot(a, b, ca, cb):
    return lax.dot_general(a, b, (((ca,), (cb,)), ((), ())), preferred_element_type=F32)


def step_kernel(
    n, inner, rows_total,
    x_hbm, wenc_hbm, wdec_hbm, benc_ref, thr_ref, bdec_ref,
    xt_hbm, et_hbm, ft_ref, gp_ref, gbenc_ref, gbdec_ref, stats_ref,
    xt, et, wenc, wdec, wdt, pre, dg, theirs, given, mine, sbuf, rbuf, st,
    load_sem, out_sem,
    a_ss, a_rs, a_ds, a_dr, r_ss, r_rs, r_ds, r_dr, e_ss, e_rs, e_ds, e_dr,
):
    blk, half = x_hbm.shape[0], x_hbm.shape[1] // 2
    depth, lat = wenc.shape
    subs = 2 if blk % 32 == 0 else 1
    sub_rows = blk // subs
    me = lax.axis_index("lat")
    core = lax.rem(me, 2)
    chip = me // 2
    m = n // 2

    if inner == 2:
        y0 = lax.rem(chip, 2)
        z0 = chip // 2
        pos = z0 + y0 * (2 * m - 1 - 2 * z0)
    else:
        pos = chip

    def chip_at(p):
        p = lax.rem(p + 2 * n, n)
        if inner == 2:
            y = p // m
            z = p + y * (2 * m - 1 - 2 * p)
            return 2 * z + y
        return p

    nxt = 2 * chip_at(pos + 1) + core
    prv = 2 * chip_at(pos - 1) + core
    mate = me + 1 - 2 * core

    barrier = pltpu.get_barrier_semaphore()
    for peer in (nxt, prv, mate):
        pl.semaphore_signal(barrier, inc=1, device_id={"lat": peer}, device_id_type=MESH)

    own_rows = pl.ds(pl.multiple_of(me * blk, 16), blk)
    load_enc = pltpu.make_async_copy(wenc_hbm, wenc, load_sem.at[0])
    load_dec = pltpu.make_async_copy(wdec_hbm, wdec, load_sem.at[1])
    load_x = [
        pltpu.make_async_copy(
            x_hbm.at[:, pl.ds(h * half, half)], xt.at[h, own_rows], load_sem.at[2 + h]
        )
        for h in range(2)
    ]
    for h in range(2):
        load_x[h].start()
    load_enc.start()
    load_dec.start()
    for h in range(2):
        load_x[h].wait()
    pl.semaphore_wait(barrier, 3)

    def remote(src, dst, ss, rs, peer):
        return pltpu.make_async_remote_copy(
            src_ref=src, dst_ref=dst, send_sem=ss, recv_sem=rs,
            device_id={"lat": peer}, device_id_type=MESH,
        )

    def make_gather(buf, with_stats, ss, rs, ds, dr):
        flows = [(h, u) for u in range(subs) for h in range(2)]
        if with_stats:
            flows.append((0, -1))

        def piece(f, dev):
            h, u = flows[f]
            if u < 0:
                return st.at[dev]
            return buf.at[h, pl.ds(pl.multiple_of(dev * blk + u * sub_rows, 16), sub_rows)]

        def dev_at(f, s, c):
            sign = 1 if flows[f][0] == 0 else -1
            return 2 * chip_at(pos - sign * s) + c

        def ring(f, s):
            r = piece(f, dev_at(f, s, core))
            return remote(r, r, ss.at[f, s], rs.at[f, s], nxt if flows[f][0] == 0 else prv)

        def ring_in(f, s):
            r = piece(f, dev_at(f, s + 1, core))
            return remote(r, r, ss.at[f, s], rs.at[f, s], nxt if flows[f][0] == 0 else prv)

        def d2d(f, s):
            r = piece(f, dev_at(f, s, core))
            return remote(r, r, ds.at[f, s], dr.at[f, s], mate)

        def d2d_in(f, s):
            r = piece(f, dev_at(f, s, 1 - core))
            return remote(r, r, ds.at[f, s], dr.at[f, s], mate)

        count = range(len(flows))

        def run(first, compute):
            for f in count:
                ring(f, 0).start()
            for f in count:
                d2d(f, 0).start()

            def arrive(s):
                for f in count:
                    d2d_in(f, s).wait_recv()

            def forward(s):
                for f in count:
                    ring_in(f, s - 1).wait_recv()
                    ring(f, s).start()
                    d2d(f, s).start()
                arrive(s - 1)

            forward(1)
            first()
            compute(0)

            @pl.loop(2, n - 1)
            def _(s):
                forward(s)
                compute(s - 1)

            for f in count:
                ring_in(f, n - 2).wait_recv()
                d2d(f, n - 1).start()
            arrive(n - 2)
            compute(n - 2)
            arrive(n - 1)
            compute(n - 1)

            @pl.loop(0, n - 1)
            def _(s):
                for f in count:
                    ring(f, s).wait_send()

            @pl.loop(0, n)
            def _(s):
                for f in count:
                    d2d(f, s).wait_send()

        return run

    def first():
        pre[...] = jnp.zeros_like(pre)
        load_enc.wait()
        load_dec.wait()

    slices = depth // 128
    each = pl.cdiv(slices, n)

    def encode(s):
        @pl.loop(s * each, jnp.minimum((s + 1) * each, slices))
        def _(i):
            c = pl.ds(pl.multiple_of(i * 128, 128), 128)
            wdt[c, :] = wdec[:, c].T

        for h in range(2):
            q = chip_at(pos - s if h == 0 else pos + s)
            r = pl.ds(pl.multiple_of(q * 2 * blk, 16), 2 * blk)
            pre[h] += dot(wenc[r, :], xt[h, r, :], 0, 0)

    make_gather(xt, False, a_ss, a_rs, a_ds, a_dr)(first, encode)
    out_x = pltpu.make_async_copy(xt, xt_hbm, out_sem.at[0])
    out_x.start()

    benc = jnp.broadcast_to(benc_ref[...], (128, lat)).T[:, :1]
    thr = jnp.broadcast_to(thr_ref[...], (128, lat)).T[:, :1]
    bdec = jnp.broadcast_to(bdec_ref[...].astype(F32), (128, blk)).T[:, :1]
    total = jnp.zeros((1, half), F32)
    for h in range(2):
        p = pre[h] + benc
        gate = jax.nn.sigmoid((p - thr) / 0.05)
        ft_ref[h] = (p * gate).astype(BF16)
        dg[h] = gate + p * gate * (1.0 - gate) / 0.05
        total = total + jnp.sum(gate, axis=0, keepdims=True)

    def block_at(h, t):
        return chip_at(pos - 1 - t if h == 0 else pos + 1 + t)

    def swap(h, t):
        return remote(theirs.at[h, t], given.at[h, t], r_ds.at[h, t], r_dr.at[h, t], mate)

    def partial(t):
        for h in range(2):
            q = block_at(h, t)
            other = pl.ds(pl.multiple_of((2 * q + 1 - core) * blk, 16), blk)
            theirs[h, t] = dot(wdt[other, :], ft_ref[h], 1, 0).astype(BF16)
            swap(h, t).start()
        for h in range(2):
            q = block_at(h, t)
            same = pl.ds(pl.multiple_of((2 * q + core) * blk, 16), blk)
            mine[h, t] = dot(wdt[same, :], ft_ref[h], 1, 0)

    def pass_on(h, u, s):
        r = pl.ds(u * sub_rows, sub_rows)
        f = h * subs + u
        return remote(
            sbuf.at[h, s, r], rbuf.at[h, s, r], r_ss.at[f, s], r_rs.at[f, s], nxt if h == 0 else prv
        )

    def hop(s, has_input):
        for h in range(2):
            swap(h, s).wait_recv()
        for u in range(subs):
            for h in range(2):
                r = pl.ds(u * sub_rows, sub_rows)
                v = mine[h, s, r, :] + given[h, s, r, :].astype(F32)
                if has_input:
                    pass_on(h, u, s - 1).wait_recv()
                    v = v + rbuf[h, s - 1, r, :].astype(F32)
                sbuf[h, s, r, :] = v.astype(BF16)
                pass_on(h, u, s).start()

    partial(0)
    partial(1)
    hop(0, False)
    partial(2)

    @pl.loop(1, n - 2)
    def _(s):
        hop(s, True)
        partial(s + 2)

    hop(n - 2, True)
    sq = jnp.zeros((1, half), F32)
    gb = jnp.zeros((blk, 1), F32)
    for h in range(2):
        swap(h, n - 1).wait_recv()
        for u in range(subs):
            pass_on(h, u, n - 2).wait_recv()
        recon = mine[h, n - 1] + given[h, n - 1].astype(F32) + rbuf[h, n - 2].astype(F32) + bdec
        err = recon - xt[h, own_rows, :].astype(F32)
        scaled = (2.0 / rows_total) * err
        et[h, own_rows, :] = scaled.astype(BF16)
        sq = sq + jnp.sum(err * err, axis=0, keepdims=True)
        gb = gb + jnp.sum(scaled, axis=1, keepdims=True)
    gbdec_ref[...] = jnp.broadcast_to(gb, (blk, 128)).T[:1]
    lane = lax.broadcasted_iota(jnp.int32, (8, 128), 0)
    st[me] = jnp.where(lane == 0, jnp.sum(sq), jnp.sum(total))

    def clear():
        pre[...] = jnp.zeros_like(pre)

    def decode_back(s):
        for h in range(2):
            q = chip_at(pos - s if h == 0 else pos + s)
            r = pl.ds(pl.multiple_of(q * 2 * blk, 16), 2 * blk)
            pre[h] += dot(wdt[r, :], et[h, r, :], 0, 0)

    make_gather(et, True, e_ss, e_rs, e_ds, e_dr)(clear, decode_back)
    out_e = pltpu.make_async_copy(et, et_hbm, out_sem.at[1])
    out_e.start()

    @pl.loop(0, n - 1)
    def _(s):
        for h in range(2):
            for u in range(subs):
                pass_on(h, u, s).wait_send()

    @pl.loop(0, n)
    def _(s):
        for h in range(2):
            swap(h, s).wait_send()

    gsum = jnp.zeros((lat, 1), F32)
    for h in range(2):
        g = pre[h] * dg[h]
        gp_ref[h] = g.astype(BF16)
        gsum = gsum + jnp.sum(g, axis=1, keepdims=True)
    gbenc_ref[...] = jnp.broadcast_to(gsum, (lat, 128)).T[:1]
    stats_ref[...] = jnp.sum(st[...], axis=0)
    out_x.wait()
    out_e.wait()


def grads_kernel(
    sq_scale, gate_scale,
    xt_ref, et_ref, ft_ref, gp_ref, gbenc_in, gbdec_in, stats_ref, spars_ref,
    genc_ref, gdec_ref, gbenc_ref, gbdec_ref, loss_ref,
):
    genc_ref[...] = (dot(xt_ref[0], gp_ref[0], 1, 1) + dot(xt_ref[1], gp_ref[1], 1, 1)).astype(BF16)
    gdec_ref[...] = (dot(ft_ref[0], et_ref[0], 1, 1) + dot(ft_ref[1], et_ref[1], 1, 1)).astype(BF16)

    @pl.when(pl.program_id(0) == 0)
    def _():
        gbenc_ref[...] = gbenc_in[...]
        gbdec_ref[...] = gbdec_in[...]
        at = lax.broadcasted_iota(jnp.int32, (8, 128), 0)
        lane = lax.broadcasted_iota(jnp.int32, (8, 128), 1)
        v = stats_ref[...]
        loss_ref[0] = jnp.sum(jnp.where((at == 0) & (lane == 0), v, 0.0)) * sq_scale
        count = jnp.sum(jnp.where((at == 1) & (lane == 0), v, 0.0))
        loss_ref[1] = spars_ref[0] * count * gate_scale


def on_device(inner, inputs, w_enc, b_enc, thresholds, w_dec, b_dec, sparsity):
    rows, blk = inputs.shape
    parts = lax.axis_size("lat")
    n = parts // 2
    depth, lat = w_enc.shape
    half = rows // 2
    subs = 2 if blk % 32 == 0 else 1
    nf = 2 * subs
    vmem = pl.BlockSpec(memory_space=pltpu.VMEM)
    hbm = pl.BlockSpec(memory_space=pl.ANY)
    dma = pltpu.SemaphoreType.DMA
    xt, et, ft, gp, gbenc, gbdec, stats = pl.pallas_call(
        functools.partial(step_kernel, n, inner, rows),
        out_shape=(
            jax.ShapeDtypeStruct((2, depth, half), BF16),
            jax.ShapeDtypeStruct((2, depth, half), BF16),
            jax.ShapeDtypeStruct((2, lat, half), BF16),
            jax.ShapeDtypeStruct((2, lat, half), BF16),
            jax.ShapeDtypeStruct((1, lat), F32),
            jax.ShapeDtypeStruct((1, blk), F32),
            jax.ShapeDtypeStruct((8, 128), F32),
        ),
        in_specs=[hbm, hbm, hbm, vmem, vmem, vmem],
        out_specs=(hbm, hbm, vmem, vmem, vmem, vmem, vmem),
        scratch_shapes=[
            pltpu.VMEM((2, depth, half), BF16),
            pltpu.VMEM((2, depth, half), BF16),
            pltpu.VMEM((depth, lat), BF16),
            pltpu.VMEM((lat, depth), BF16),
            pltpu.VMEM((depth, lat), BF16),
            pltpu.VMEM((2, lat, half), F32),
            pltpu.VMEM((2, lat, half), F32),
            pltpu.VMEM((2, n, blk, half), BF16),
            pltpu.VMEM((2, n, blk, half), BF16),
            pltpu.VMEM((2, n, blk, half), F32),
            pltpu.VMEM((2, n - 1, blk, half), BF16),
            pltpu.VMEM((2, n - 1, blk, half), BF16),
            pltpu.VMEM((parts, 8, 128), F32),
            dma((4,)),
            dma((2,)),
            dma((nf, n - 1)), dma((nf, n - 1)), dma((nf, n)), dma((nf, n)),
            dma((nf, n - 1)), dma((nf, n - 1)), dma((2, n)), dma((2, n)),
            dma((nf + 1, n - 1)), dma((nf + 1, n - 1)), dma((nf + 1, n)), dma((nf + 1, n)),
        ],
        compiler_params=pltpu.CompilerParams(
            collective_id=0, has_side_effects=True, vmem_limit_bytes=63 * 1024 * 1024
        ),
        name="sae_step",
    )(
        inputs.T, w_enc, w_dec, b_enc.reshape(1, lat), thresholds.reshape(1, lat),
        b_dec.reshape(1, blk),
    )
    tile = 512 if depth % 512 == 0 else 128
    row = lambda width: pl.BlockSpec((1, width), lambda i: (0, 0))
    smem = pl.BlockSpec(memory_space=pltpu.SMEM)
    grad_enc, grad_dec, grad_b_enc, grad_b_dec, loss_terms = pl.pallas_call(
        functools.partial(grads_kernel, 1.0 / (rows * depth), 1.0 / (rows * lat * parts)),
        grid=(depth // tile,),
        out_shape=(
            jax.ShapeDtypeStruct((depth, lat), BF16),
            jax.ShapeDtypeStruct((lat, depth), BF16),
            jax.ShapeDtypeStruct((1, lat), F32),
            jax.ShapeDtypeStruct((1, blk), F32),
            jax.ShapeDtypeStruct((2,), F32),
        ),
        in_specs=[
            pl.BlockSpec((2, tile, half), lambda i: (0, i, 0)),
            pl.BlockSpec((2, tile, half), lambda i: (0, i, 0)),
            pl.BlockSpec((2, lat, half), lambda i: (0, 0, 0)),
            pl.BlockSpec((2, lat, half), lambda i: (0, 0, 0)),
            row(lat),
            row(blk),
            pl.BlockSpec((8, 128), lambda i: (0, 0)),
            smem,
        ],
        out_specs=(
            pl.BlockSpec((tile, lat), lambda i: (i, 0)),
            pl.BlockSpec((lat, tile), lambda i: (0, i)),
            row(lat),
            row(blk),
            smem,
        ),
        name="sae_grads",
    )(xt, et, ft, gp, gbenc, gbdec, stats, sparsity)
    return grad_enc, grad_b_enc.reshape(lat), grad_dec, grad_b_dec.reshape(blk), loss_terms


def chips_inner(mesh):
    try:
        where = [tuple(d.coords) for d in mesh.devices.reshape(-1, mesh.shape["lat"])[0][::2]]
    except AttributeError:
        return 1
    if len(where) < 4 or len(where) % 2:
        return 1
    moved = [sum(a != b for a, b in zip(where[0], w)) for w in (where[1], where[2], where[3])]
    return 2 if moved == [1, 1, 2] else 1


def solution(mesh):
    return jax.shard_map(
        functools.partial(on_device, chips_inner(mesh)),
        mesh=mesh,
        in_specs=(
            P("groups", "lat"),
            P("groups", "lat"),
            P(("groups", "lat")),
            P(("groups", "lat")),
            P(("groups", "lat"), None),
            P(("groups", "lat")),
            P("groups"),
        ),
        out_specs=(
            P("groups", "lat"),
            P(("groups", "lat")),
            P(("groups", "lat"), None),
            P(("groups", "lat")),
            P("groups"),
        ),
        check_vma=False,
    )
```

```python
import functools

import jax
import jax.numpy as jnp
from jax import lax
from jax.experimental import pallas as pl
from jax.experimental.pallas import tpu as pltpu
from jax.sharding import PartitionSpec as P

MESH = pl.DeviceIdType.MESH
F32 = jnp.float32
BF16 = jnp.bfloat16


def dot(a, b, ca, cb):
    return lax.dot_general(a, b, (((ca,), (cb,)), ((), ())), preferred_element_type=F32)


def step_kernel(
    n, inner, rows_total,
    x_hbm, wenc_hbm, wdec_hbm, benc_ref, thr_ref, bdec_ref,
    xt, et, ft_ref, gp_ref, gbenc_ref, gbdec_ref, stats_ref,
    wenc, wdec, wdt, pre, dg, theirs, given, mine, sbuf, rbuf, st,
    load_sem,
    a_ss, a_rs, a_ds, a_dr, r_ss, r_rs, r_ds, r_dr, e_ss, e_rs, e_ds, e_dr,
):
    blk, half = x_hbm.shape[0], x_hbm.shape[1] // 2
    depth, lat = wenc.shape
    subs = 2 if blk % 32 == 0 else 1
    sub_rows = blk // subs
    me = lax.axis_index("lat")
    core = lax.rem(me, 2)
    chip = me // 2
    m = n // 2

    if inner == 2:
        y0 = lax.rem(chip, 2)
        z0 = chip // 2
        pos = z0 + y0 * (2 * m - 1 - 2 * z0)
    else:
        pos = chip

    def chip_at(p):
        p = lax.rem(p + 2 * n, n)
        if inner == 2:
            y = p // m
            z = p + y * (2 * m - 1 - 2 * p)
            return 2 * z + y
        return p

    nxt = 2 * chip_at(pos + 1) + core
    prv = 2 * chip_at(pos - 1) + core
    mate = me + 1 - 2 * core

    barrier = pltpu.get_barrier_semaphore()
    for peer in (nxt, prv, mate):
        pl.semaphore_signal(barrier, inc=1, device_id={"lat": peer}, device_id_type=MESH)

    own_rows = pl.ds(pl.multiple_of(me * blk, 16), blk)
    load_enc = pltpu.make_async_copy(wenc_hbm, wenc, load_sem.at[0])
    load_dec = pltpu.make_async_copy(wdec_hbm, wdec, load_sem.at[1])
    load_x = [
        pltpu.make_async_copy(
            x_hbm.at[:, pl.ds(h * half, half)], xt.at[h, own_rows], load_sem.at[2 + h]
        )
        for h in range(2)
    ]
    for h in range(2):
        load_x[h].start()
    load_enc.start()
    load_dec.start()
    for h in range(2):
        load_x[h].wait()
    pl.semaphore_wait(barrier, 3)

    def remote(src, dst, ss, rs, peer):
        return pltpu.make_async_remote_copy(
            src_ref=src, dst_ref=dst, send_sem=ss, recv_sem=rs,
            device_id={"lat": peer}, device_id_type=MESH,
        )

    def make_gather(buf, with_stats, ss, rs, ds, dr):
        flows = [(h, u) for u in range(subs) for h in range(2)]
        if with_stats:
            flows.append((0, -1))

        def piece(f, dev):
            h, u = flows[f]
            if u < 0:
                return st.at[dev]
            return buf.at[h, pl.ds(pl.multiple_of(dev * blk + u * sub_rows, 16), sub_rows)]

        def dev_at(f, s, c):
            sign = 1 if flows[f][0] == 0 else -1
            return 2 * chip_at(pos - sign * s) + c

        def ring(f, s):
            r = piece(f, dev_at(f, s, core))
            return remote(r, r, ss.at[f, s], rs.at[f, s], nxt if flows[f][0] == 0 else prv)

        def ring_in(f, s):
            r = piece(f, dev_at(f, s + 1, core))
            return remote(r, r, ss.at[f, s], rs.at[f, s], nxt if flows[f][0] == 0 else prv)

        def d2d(f, s):
            r = piece(f, dev_at(f, s, core))
            return remote(r, r, ds.at[f, s], dr.at[f, s], mate)

        def d2d_in(f, s):
            r = piece(f, dev_at(f, s, 1 - core))
            return remote(r, r, ds.at[f, s], dr.at[f, s], mate)

        count = range(len(flows))

        def run(first, compute):
            for f in count:
                ring(f, 0).start()
            for f in count:
                d2d(f, 0).start()

            def arrive(s):
                for f in count:
                    d2d_in(f, s).wait_recv()

            def forward(s):
                for f in count:
                    ring_in(f, s - 1).wait_recv()
                    ring(f, s).start()
                    d2d(f, s).start()
                arrive(s - 1)

            forward(1)
            first()
            compute(0)

            @pl.loop(2, n - 1)
            def _(s):
                forward(s)
                compute(s - 1)

            for f in count:
                ring_in(f, n - 2).wait_recv()
                d2d(f, n - 1).start()
            arrive(n - 2)
            compute(n - 2)
            arrive(n - 1)
            compute(n - 1)

            @pl.loop(0, n - 1)
            def _(s):
                for f in count:
                    ring(f, s).wait_send()

            @pl.loop(0, n)
            def _(s):
                for f in count:
                    d2d(f, s).wait_send()

        return run

    def first():
        pre[...] = jnp.zeros_like(pre)
        load_enc.wait()
        load_dec.wait()

    slices = depth // 128
    each = pl.cdiv(slices, n)

    def encode(s):
        @pl.loop(s * each, jnp.minimum((s + 1) * each, slices))
        def _(i):
            c = pl.ds(pl.multiple_of(i * 128, 128), 128)
            wdt[c, :] = wdec[:, c].T

        for h in range(2):
            q = chip_at(pos - s if h == 0 else pos + s)
            r = pl.ds(pl.multiple_of(q * 2 * blk, 16), 2 * blk)
            pre[h] += dot(wenc[r, :], xt[h, r, :], 0, 0)

    make_gather(xt, False, a_ss, a_rs, a_ds, a_dr)(first, encode)

    benc = jnp.broadcast_to(benc_ref[...], (128, lat)).T[:, :1]
    thr = jnp.broadcast_to(thr_ref[...], (128, lat)).T[:, :1]
    bdec = jnp.broadcast_to(bdec_ref[...].astype(F32), (128, blk)).T[:, :1]
    total = jnp.zeros((1, half), F32)
    for h in range(2):
        p = pre[h] + benc
        gate = jax.nn.sigmoid((p - thr) / 0.05)
        ft_ref[h] = (p * gate).astype(BF16)
        dg[h] = gate + p * gate * (1.0 - gate) / 0.05
        total = total + jnp.sum(gate, axis=0, keepdims=True)

    def block_at(h, t):
        return chip_at(pos - 1 - t if h == 0 else pos + 1 + t)

    def swap(h, t):
        return remote(theirs.at[h, t], given.at[h, t], r_ds.at[h, t], r_dr.at[h, t], mate)

    def partial(t):
        for h in range(2):
            q = block_at(h, t)
            other = pl.ds(pl.multiple_of((2 * q + 1 - core) * blk, 16), blk)
            theirs[h, t] = dot(wdt[other, :], ft_ref[h], 1, 0).astype(BF16)
            swap(h, t).start()
        for h in range(2):
            q = block_at(h, t)
            same = pl.ds(pl.multiple_of((2 * q + core) * blk, 16), blk)
            mine[h, t] = dot(wdt[same, :], ft_ref[h], 1, 0)

    def pass_on(h, u, s):
        r = pl.ds(u * sub_rows, sub_rows)
        f = h * subs + u
        return remote(
            sbuf.at[h, s, r], rbuf.at[h, s, r], r_ss.at[f, s], r_rs.at[f, s], nxt if h == 0 else prv
        )

    def hop(s, has_input):
        for h in range(2):
            swap(h, s).wait_recv()
        for u in range(subs):
            for h in range(2):
                r = pl.ds(u * sub_rows, sub_rows)
                v = mine[h, s, r, :] + given[h, s, r, :].astype(F32)
                if has_input:
                    pass_on(h, u, s - 1).wait_recv()
                    v = v + rbuf[h, s - 1, r, :].astype(F32)
                sbuf[h, s, r, :] = v.astype(BF16)
                pass_on(h, u, s).start()

    partial(0)
    partial(1)
    hop(0, False)
    partial(2)

    @pl.loop(1, n - 2)
    def _(s):
        hop(s, True)
        partial(s + 2)

    hop(n - 2, True)
    sq = jnp.zeros((1, half), F32)
    gb = jnp.zeros((blk, 1), F32)
    for h in range(2):
        swap(h, n - 1).wait_recv()
        for u in range(subs):
            pass_on(h, u, n - 2).wait_recv()
        recon = mine[h, n - 1] + given[h, n - 1].astype(F32) + rbuf[h, n - 2].astype(F32) + bdec
        err = recon - xt[h, own_rows, :].astype(F32)
        scaled = (2.0 / rows_total) * err
        et[h, own_rows, :] = scaled.astype(BF16)
        sq = sq + jnp.sum(err * err, axis=0, keepdims=True)
        gb = gb + jnp.sum(scaled, axis=1, keepdims=True)
    gbdec_ref[...] = jnp.broadcast_to(gb, (blk, 128)).T[:1]
    lane = lax.broadcasted_iota(jnp.int32, (8, 128), 0)
    st[me] = jnp.where(lane == 0, jnp.sum(sq), jnp.sum(total))

    def clear():
        pre[...] = jnp.zeros_like(pre)

    def decode_back(s):
        for h in range(2):
            q = chip_at(pos - s if h == 0 else pos + s)
            r = pl.ds(pl.multiple_of(q * 2 * blk, 16), 2 * blk)
            pre[h] += dot(wdt[r, :], et[h, r, :], 0, 0)

    make_gather(et, True, e_ss, e_rs, e_ds, e_dr)(clear, decode_back)

    @pl.loop(0, n - 1)
    def _(s):
        for h in range(2):
            for u in range(subs):
                pass_on(h, u, s).wait_send()

    @pl.loop(0, n)
    def _(s):
        for h in range(2):
            swap(h, s).wait_send()

    gsum = jnp.zeros((lat, 1), F32)
    for h in range(2):
        g = pre[h] * dg[h]
        gp_ref[h] = g.astype(BF16)
        gsum = gsum + jnp.sum(g, axis=1, keepdims=True)
    gbenc_ref[...] = jnp.broadcast_to(gsum, (lat, 128)).T[:1]
    stats_ref[...] = jnp.sum(st[...], axis=0)


def grads_kernel(
    sq_scale, gate_scale,
    xt_ref, et_ref, ft_ref, gp_ref, gbenc_in, gbdec_in, stats_ref, spars_ref,
    genc_ref, gdec_ref, gbenc_ref, gbdec_ref, loss_ref,
):
    tile = genc_ref.shape[0]
    r = pl.ds(pl.multiple_of(pl.program_id(0) * tile, 16), tile)
    genc_ref[...] = (
        dot(xt_ref[0, r, :], gp_ref[0], 1, 1) + dot(xt_ref[1, r, :], gp_ref[1], 1, 1)
    ).astype(BF16)
    gdec_ref[...] = (
        dot(ft_ref[0], et_ref[0, r, :], 1, 1) + dot(ft_ref[1], et_ref[1, r, :], 1, 1)
    ).astype(BF16)

    @pl.when(pl.program_id(0) == 0)
    def _():
        gbenc_ref[...] = gbenc_in[...]
        gbdec_ref[...] = gbdec_in[...]
        at = lax.broadcasted_iota(jnp.int32, (8, 128), 0)
        lane = lax.broadcasted_iota(jnp.int32, (8, 128), 1)
        v = stats_ref[...]
        loss_ref[0] = jnp.sum(jnp.where((at == 0) & (lane == 0), v, 0.0)) * sq_scale
        count = jnp.sum(jnp.where((at == 1) & (lane == 0), v, 0.0))
        loss_ref[1] = spars_ref[0] * count * gate_scale


def on_device(inner, inputs, w_enc, b_enc, thresholds, w_dec, b_dec, sparsity):
    rows, blk = inputs.shape
    parts = lax.axis_size("lat")
    n = parts // 2
    depth, lat = w_enc.shape
    half = rows // 2
    subs = 2 if blk % 32 == 0 else 1
    nf = 2 * subs
    vmem = pl.BlockSpec(memory_space=pltpu.VMEM)
    hbm = pl.BlockSpec(memory_space=pl.ANY)
    dma = pltpu.SemaphoreType.DMA
    xt, et, ft, gp, gbenc, gbdec, stats = pl.pallas_call(
        functools.partial(step_kernel, n, inner, rows),
        out_shape=(
            pltpu.VMEM((2, depth, half), BF16),
            pltpu.VMEM((2, depth, half), BF16),
            pltpu.VMEM((2, lat, half), BF16),
            pltpu.VMEM((2, lat, half), BF16),
            jax.ShapeDtypeStruct((1, lat), F32),
            jax.ShapeDtypeStruct((1, blk), F32),
            jax.ShapeDtypeStruct((8, 128), F32),
        ),
        in_specs=[hbm, hbm, hbm, vmem, vmem, vmem],
        out_specs=(vmem, vmem, vmem, vmem, vmem, vmem, vmem),
        scratch_shapes=[
            pltpu.VMEM((depth, lat), BF16),
            pltpu.VMEM((lat, depth), BF16),
            pltpu.VMEM((depth, lat), BF16),
            pltpu.VMEM((2, lat, half), F32),
            pltpu.VMEM((2, lat, half), F32),
            pltpu.VMEM((2, n, blk, half), BF16),
            pltpu.VMEM((2, n, blk, half), BF16),
            pltpu.VMEM((2, n, blk, half), F32),
            pltpu.VMEM((2, n - 1, blk, half), BF16),
            pltpu.VMEM((2, n - 1, blk, half), BF16),
            pltpu.VMEM((parts, 8, 128), F32),
            dma((4,)),
            dma((nf, n - 1)), dma((nf, n - 1)), dma((nf, n)), dma((nf, n)),
            dma((nf, n - 1)), dma((nf, n - 1)), dma((2, n)), dma((2, n)),
            dma((nf + 1, n - 1)), dma((nf + 1, n - 1)), dma((nf + 1, n)), dma((nf + 1, n)),
        ],
        compiler_params=pltpu.CompilerParams(
            collective_id=0, has_side_effects=True, vmem_limit_bytes=44 * 1024 * 1024
        ),
        name="sae_step",
    )(
        inputs.T, w_enc, w_dec, b_enc.reshape(1, lat), thresholds.reshape(1, lat),
        b_dec.reshape(1, blk),
    )
    tile = 512 if depth % 512 == 0 else 128
    row = lambda width: pl.BlockSpec((1, width), lambda i: (0, 0))
    smem = pl.BlockSpec(memory_space=pltpu.SMEM)
    grad_enc, grad_dec, grad_b_enc, grad_b_dec, loss_terms = pl.pallas_call(
        functools.partial(grads_kernel, 1.0 / (rows * depth), 1.0 / (rows * lat * parts)),
        grid=(depth // tile,),
        out_shape=(
            jax.ShapeDtypeStruct((depth, lat), BF16),
            jax.ShapeDtypeStruct((lat, depth), BF16),
            jax.ShapeDtypeStruct((1, lat), F32),
            jax.ShapeDtypeStruct((1, blk), F32),
            jax.ShapeDtypeStruct((2,), F32),
        ),
        in_specs=[
            vmem,
            vmem,
            vmem,
            vmem,
            row(lat),
            row(blk),
            pl.BlockSpec((8, 128), lambda i: (0, 0)),
            smem,
        ],
        out_specs=(
            pl.BlockSpec((tile, lat), lambda i: (i, 0)),
            pl.BlockSpec((lat, tile), lambda i: (0, i)),
            row(lat),
            row(blk),
            smem,
        ),
        compiler_params=pltpu.CompilerParams(vmem_limit_bytes=16 * 1024 * 1024),
        name="sae_grads",
    )(xt, et, ft, gp, gbenc, gbdec, stats, sparsity)
    return grad_enc, grad_b_enc.reshape(lat), grad_dec, grad_b_dec.reshape(blk), loss_terms


def chips_inner(mesh):
    try:
        where = [tuple(d.coords) for d in mesh.devices.reshape(-1, mesh.shape["lat"])[0][::2]]
    except AttributeError:
        return 1
    if len(where) < 4 or len(where) % 2:
        return 1
    moved = [sum(a != b for a, b in zip(where[0], w)) for w in (where[1], where[2], where[3])]
    return 2 if moved == [1, 1, 2] else 1


def solution(mesh):
    return jax.shard_map(
        functools.partial(on_device, chips_inner(mesh)),
        mesh=mesh,
        in_specs=(
            P("groups", "lat"),
            P("groups", "lat"),
            P(("groups", "lat")),
            P(("groups", "lat")),
            P(("groups", "lat"), None),
            P(("groups", "lat")),
            P("groups"),
        ),
        out_specs=(
            P("groups", "lat"),
            P(("groups", "lat")),
            P(("groups", "lat"), None),
            P(("groups", "lat")),
            P("groups"),
        ),
        check_vma=False,
    )
```
